32 devices in a mesh: ya: 8 (over z, y), zb: 4 (over x, core).
Axes of the slice: x: 2, y: 2, z: 4, core: 2. Of those that a mesh axis runs over, the one named last changes fastest.
Arguments:
- source: float32 [128, 128, 512], P(None, 'ya', 'zb'), may hold values from -6 to 6
- symbol_x: float32 [128], replicated, may hold values from 0.3 to 3
- symbol_y: float32 [128], replicated, may hold values from 0.3 to 3
- symbol_z: float32 [512], replicated, may hold values from 0.3 to 3
Outputs:
- modes: float32 [128, 128, 512], P('ya', 'zb')
The draws below stay inside these ranges and needn't reach their ends.
All inputs are finite; a program needn't handle non-finite values.
Results may differ from the reference program's by a relative error of at most 0.000071.
Values sent between devices are 32-bit elements; how exact they have to be, the bound alone decides.
A program may use at most 64 MiB of HBM per device.

```python
import jax
import jax.numpy as jnp
from jax import lax

GRID_X = 128
GRID_Y = 128
GRID_Z = 512


def block_levels(rng, shape, shards, low, top_value):
    def one(dim, parts):
        heights = jax.random.uniform(jax.random.fold_in(jax.random.fold_in(rng, 6), dim), (parts,), jnp.float32, low / len(shards), top_value / len(shards))
        return jnp.repeat(jnp.exp(heights), shape[dim] // parts).reshape((-1,) + (1,) * (len(shape) - dim - 1))

    gain = one(*shards[0])
    for cut in shards[1:]:
        gain = gain * one(*cut)
    return gain


def noise(rng, shape, width, limit, split=(), dtype=jnp.bfloat16):
    drawn = width * jax.random.normal(rng, shape, jnp.float32)
    if split:
        drawn = drawn * block_levels(rng, shape, split, -0.22, 0.18)
    return jnp.clip(drawn, -limit, limit).astype(dtype)


def setup_inputs(seed: int = 0) -> dict:
    splits = jax.random.split(jax.random.key(seed), 5)
    source = noise(splits[0], (GRID_X, GRID_Y, GRID_Z), 1.0, 6.0, ((1, 8), (2, 4)), jnp.float32)
    symbol_x = jnp.clip(jax.random.uniform(splits[1], (GRID_X,), jnp.float32, 0.3, 3.0), 0.3, 3.0)
    symbol_y = jnp.clip(jax.random.uniform(splits[2], (GRID_Y,), jnp.float32, 0.3, 3.0), 0.3, 3.0)
    symbol_z = jnp.clip(jax.random.uniform(splits[3], (GRID_Z,), jnp.float32, 0.3, 3.0), 0.3, 3.0)
    return {"source": source, "symbol_x": symbol_x, "symbol_y": symbol_y, "symbol_z": symbol_z}


def transform_table(count):
    rank = jnp.arange(count)
    angle = jnp.pi / (count + 1) * ((rank[:, None] + 1) * (rank[None, :] + 1) % (2 * count + 2)).astype(jnp.float32)
    return jnp.sin(angle) * (2.0 / (count + 1)) ** 0.5

def transform_dim(values, dim):
    moved = jnp.tensordot(values, transform_table(values.shape[dim]), axes=([dim], [0]), precision=lax.Precision.HIGHEST)
    return jnp.moveaxis(moved, -1, dim)

def reference(source, symbol_x, symbol_y, symbol_z):
    modes = source
    modes = transform_dim(modes, 0)
    modes = transform_dim(modes, 1)
    modes = transform_dim(modes, 2)
    symbol = symbol_x[:, None, None] + symbol_y[None, :, None] + symbol_z[None, None, :]
    modes = modes * lax.rsqrt(symbol)
    return modes
```

```python
import functools

import jax
import jax.numpy as jnp
import numpy as np
from jax import lax
from jax.experimental import pallas as pl
from jax.experimental.pallas import tpu as pltpu
from jax.sharding import PartitionSpec as P

MESH = pl.DeviceIdType.MESH
SHARES = (3, 3, 2, 2, 2, 2, 2)
LAG = 3
LEAD = 2
EARLY = 2
CUT = 4


def transform_table(count):
    rank = np.arange(1, count + 1)
    angle = np.pi / (count + 1) * (rank[:, None] * rank[None, :] % (2 * count + 2))
    table = np.sqrt(2.0 / (count + 1)) * np.sin(angle)
    high = table.astype(jnp.bfloat16)
    low = (table - high.astype(np.float64)).astype(jnp.bfloat16)
    return high, low


def halves(values):
    high = values.astype(jnp.bfloat16)
    return high, (values - high.astype(jnp.float32)).astype(jnp.bfloat16)


def left_product(table3, values):
    high, low = halves(values)
    stacked = jnp.concatenate([high, low, high], axis=0)
    return jnp.dot(table3, stacked, preferred_element_type=jnp.float32)


def partners(me, count):
    if count & (count - 1):
        return [lax.rem(me + step, count) for step in range(count)]
    peers, bit = [me], 1
    while bit < count:
        turn = bit * (1 - 2 * lax.rem(lax.div(me, bit), 2))
        peers += [peer + turn for peer in peers]
        bit *= 2
    return peers


def kernel(
    n_ya, n_zb, bounds,
    source, table_x, table_y, table_z, symbol_x, symbol_y, symbol_z,
    out,
    src, tx, ty, tz, sx, sy, sz, first, second, third, lines, column_x, base,
    load_sem, here_a, here_b, send_a, recv_a, send_b, recv_b,
):
    ya, zb = lax.axis_index("ya"), lax.axis_index("zb")
    nx, yl, zl = source.shape
    ny = yl * n_ya
    kl = nx // n_ya
    jl = ny // n_zb
    chunks = len(bounds) - 1
    cut = CUT if yl % CUT == 0 else yl
    to_a, to_b = partners(ya, n_ya), partners(zb, n_zb)

    barrier = pltpu.get_barrier_semaphore()

    def greet(axis, me, count):
        def one(peer, _):
            pl.semaphore_signal(barrier, inc=1, device_id={axis: peer}, device_id_type=MESH)
            return 0

        lax.fori_loop(me + 1, count, one, 0)

    greet("ya", ya, n_ya)
    greet("zb", zb, n_zb)

    rows = [pl.ds(low, cut) for low in range(0, yl, cut)]
    pairs = [(source.at[:, row], src.at[:, row]) for row in rows] + [
        (table_x, tx), (table_y, ty), (table_z, tz),
        (symbol_x, sx), (symbol_y, sy), (symbol_z, sz),
    ]
    loads = [pltpu.make_async_copy(a, b, load_sem.at[i]) for i, (a, b) in enumerate(pairs)]
    parts = len(rows)
    loads[parts].start()
    for load in loads[:parts]:
        load.start()

    flat_src = src.reshape(nx * yl, zl)
    flat_first = first.reshape(nx * yl, zl)

    def x_step(pair, _):
        values = jnp.concatenate(
            [flat_src[pl.ds(2 * pair + t, nx, stride=yl), :] for t in range(2)], axis=1
        )
        modes = left_product(tx[...], values)
        for t in range(2):
            flat_first[pl.ds(2 * pair + t, nx, stride=yl), :] = modes[:, t * zl:(t + 1) * zl]
        return 0

    def size(chunk):
        return bounds[chunk + 1] - bounds[chunk]

    def span(chunk):
        return pl.ds(bounds[chunk], size(chunk))

    def copy_a(chunk, peer, low, count):
        return pltpu.make_async_remote_copy(
            src_ref=first.at[pl.ds(peer * kl + bounds[chunk], size(chunk)), pl.ds(low, count)],
            dst_ref=second.at[
                span(chunk), pl.ds(pl.multiple_of(ya * yl + low, cut), count)
            ],
            send_sem=send_a,
            recv_sem=recv_a.at[chunk],
            device_id={"ya": peer},
            device_id_type=MESH,
        )

    order = [*range(n_ya // 2, n_ya), *range(n_ya // 2 - 1, 0, -1)]

    def each_a(todo, lower):
        for step in order:
            peer = to_a[step]
            pl.when(peer < ya if lower else peer > ya)(functools.partial(todo, peer))

    def copy_b(chunk, step):
        peer = to_b[step]
        return pltpu.make_async_remote_copy(
            src_ref=third.at[span(chunk), pl.ds(pl.multiple_of(peer * jl, jl), jl)],
            dst_ref=lines.at[zb, span(chunk)],
            send_sem=send_b,
            recv_sem=recv_b.at[chunk],
            device_id={"zb": peer},
            device_id_type=MESH,
        )

    def all_of(ref, sem):
        return pltpu.make_async_copy(ref, ref, sem)

    pl.when(ya + zb > 0)(lambda: pl.semaphore_wait(barrier, ya + zb))

    def answer(peer, _):
        pl.semaphore_signal(here_a.at[ya], inc=1, device_id={"ya": peer}, device_id_type=MESH)
        return 0

    def answer_b(peer, _):
        pl.semaphore_signal(here_b, inc=1, device_id={"zb": peer}, device_id_type=MESH)
        return 0

    lax.fori_loop(0, ya, answer, 0)
    lax.fori_loop(0, zb, answer_b, 0)

    for part in range(parts):
        if part == 0:
            loads[parts].wait()
            loads[part].wait()
            for load in loads[parts + 1:]:
                load.start()
        else:
            loads[part].wait()
        lax.fori_loop(part * cut // 2, (part + 1) * cut // 2, x_step, 0, unroll=True)
        each_a(lambda peer: copy_a(0, peer, part * cut, cut).start(), True)

    def serve(chunk, peer):
        copy_a(chunk, peer, 0, yl).start()

    for chunk in range(1, min(LEAD + 1, chunks)):
        pl.when(ya > 0)(functools.partial(serve, chunk, 0))
    for chunk in range(1, chunks):
        if chunk + LEAD < chunks:
            pl.when(ya > 0)(functools.partial(serve, chunk + LEAD, 0))
        each_a(lambda peer: pl.when(peer > 0)(functools.partial(serve, chunk, peer)), True)

    for peer in range(1, n_ya):
        @pl.when(peer > ya)
        def _():
            pl.semaphore_wait(here_a.at[peer], 1)
            for part in range(parts):
                copy_a(0, peer, part * cut, cut).start()
            for chunk in range(1, min(EARLY, chunks)):
                serve(chunk, peer)
    for chunk in range(EARLY, chunks):
        each_a(functools.partial(serve, chunk), False)

    second[:, pl.ds(pl.multiple_of(ya * yl, yl), yl), :] = first[pl.ds(ya * kl, kl)]

    for load in loads[parts + 1:]:
        load.wait()

    def column(row):
        return jnp.broadcast_to(row, (zl, row.shape[1])).T

    column_x[...] = column(sx[...])
    third[0] = column(sy[...])
    own_y = third[0, pl.ds(pl.multiple_of(zb * jl, jl), jl), :]
    base[...] = jnp.concatenate([own_y] * n_zb, axis=1) + sz[...]
    above = n_zb - 1 - zb
    pl.when(above > 0)(lambda: pl.semaphore_wait(here_b, above))

    def y_stage(chunk):
        all_of(second.at[span(chunk), pl.ds(0, ny - yl)], recv_a.at[chunk]).wait()
        for low in range(bounds[chunk], bounds[chunk + 1], 2):
            planes = range(low, min(low + 2, bounds[chunk + 1]))
            values = jnp.concatenate([second[k] for k in planes], axis=1)
            modes = left_product(ty[...], values)
            for t, k in enumerate(planes):
                third[k] = modes[:, t * zl:(t + 1) * zl]
        for step in range(n_zb - 1, 0, -1):
            copy_b(chunk, step).start()
        lines[zb, span(chunk)] = third[
            span(chunk), pl.ds(pl.multiple_of(zb * jl, jl), jl), :
        ]

    def z_stage(chunk):
        all_of(third.at[span(chunk), pl.ds(0, ny - jl)], recv_b.at[chunk]).wait()
        values = jnp.concatenate(
            [lines[b, span(chunk)].reshape(size(chunk) * jl, zl) for b in range(n_zb)], axis=1
        )
        high, low = halves(values)
        dot = functools.partial(jnp.dot, preferred_element_type=jnp.float32)
        both = dot(jnp.concatenate([high, low], axis=0), tz[0])
        rows = high.shape[0]
        modes = both[:rows] + both[rows:] + dot(high, tz[1])
        for t in range(size(chunk)):
            k = bounds[chunk] + t
            own_x = jnp.concatenate([column_x[pl.ds(ya * kl + k, 1), :]] * n_zb, axis=1)
            out[k] = modes[t * jl:(t + 1) * jl] * lax.rsqrt(base[...] + own_x)

    for turn in range(chunks + LAG):
        if turn < chunks:
            y_stage(turn)
        if turn >= LAG:
            z_stage(turn - LAG)

    all_of(first.at[pl.ds(0, nx - kl)], send_a).wait()
    all_of(third.at[:, pl.ds(0, ny - jl)], send_b).wait()


def body(n_ya, n_zb, source, symbol_x, symbol_y, symbol_z):
    nx, yl, zl = source.shape
    ny, nz = yl * n_ya, zl * n_zb
    kl, jl = nx // n_ya, ny // n_zb
    ends = np.cumsum(SHARES) * kl // sum(SHARES)
    bounds = tuple(sorted({0, *ends.tolist()}))
    chunks = len(bounds) - 1
    tables = []
    for count in (nx, ny):
        high, low = transform_table(count)
        tables.append(np.concatenate([high, high, low], axis=1))
    tables.append(np.stack(transform_table(nz)))
    room = 67_043_328 - 4 * kl * jl * nz - 2**18
    dma = pltpu.SemaphoreType.DMA
    regular = pltpu.SemaphoreType.REGULAR
    vmem = pltpu.VMEM
    return pl.pallas_call(
        functools.partial(kernel, n_ya, n_zb, bounds),
        out_shape=pltpu.VMEM((kl, jl, nz), jnp.float32),
        in_specs=[pl.BlockSpec(memory_space=pltpu.HBM)] * 7,
        out_specs=pl.BlockSpec(memory_space=pltpu.VMEM),
        scratch_shapes=[
            vmem((nx, yl, zl), jnp.float32),
            vmem((nx, 3 * nx), jnp.bfloat16),
            vmem((ny, 3 * ny), jnp.bfloat16),
            vmem((2, nz, nz), jnp.bfloat16),
            vmem((1, nx), jnp.float32),
            vmem((1, ny), jnp.float32),
            vmem((1, nz), jnp.float32),
            vmem((nx, yl, zl), jnp.float32),
            vmem((kl, ny, zl), jnp.float32),
            vmem((kl, ny, zl), jnp.float32),
            vmem((n_zb, kl, jl, zl), jnp.float32),
            vmem((nx, zl), jnp.float32),
            vmem((jl, nz), jnp.float32),
            dma((6 + (yl // CUT if yl % CUT == 0 else 1),)),
            regular((n_ya,)),
            regular,
            dma,
            dma((chunks,)),
            dma,
            dma((chunks,)),
        ],
        compiler_params=pltpu.CompilerParams(
            collective_id=0, has_side_effects=True, vmem_limit_bytes=room
        ),
    )(
        source, *[jnp.asarray(t) for t in tables],
        symbol_x[None], symbol_y[None], symbol_z[None],
    )


def solution(mesh):
    placed = (P(None, "ya", "zb"), P(), P(), P())
    return jax.shard_map(
        functools.partial(body, mesh.shape["ya"], mesh.shape["zb"]),
        mesh=mesh, in_specs=placed, out_specs=P("ya", "zb", None), check_vma=False,
    )
```

```python
import functools
import math

import jax
import jax.numpy as jnp
import numpy as np
from jax import lax
from jax.experimental import pallas as pl
from jax.experimental.pallas import tpu as pltpu
from jax.sharding import PartitionSpec as P

MESH = pl.DeviceIdType.MESH
SHARES = (3, 3, 2, 2, 2, 2, 2)
LAG = 3
PIECES = 4
LEAD = 2
LATE = 3
BEHIND = 2
DIRECT = 2
CUTS = (2, 8)
BARPOS = 0
EARLY = 3
BEYOND = (2, 4, 6)


def transform_table(count):
    rank = np.arange(1, count + 1)
    angle = np.pi / (count + 1) * (rank[:, None] * rank[None, :] % (2 * count + 2))
    table = np.sqrt(2.0 / (count + 1)) * np.sin(angle)
    high = table.astype(jnp.bfloat16)
    low = (table - high.astype(np.float64)).astype(jnp.bfloat16)
    return high, low


def halves(values):
    high = values.astype(jnp.bfloat16)
    return high, (values - high.astype(jnp.float32)).astype(jnp.bfloat16)


def left_product(table3, values):
    high, low = halves(values)
    stacked = jnp.concatenate([high, low, high], axis=0)
    return jnp.dot(table3, stacked, preferred_element_type=jnp.float32)


def right_product(lines, planes, table):
    parts = [lines[b, planes] for b in range(lines.shape[0])]
    rows = parts[0].shape[0] * parts[0].shape[1]
    values = jnp.concatenate([part.reshape(rows, part.shape[2]) for part in parts], axis=1)
    high, low = halves(values)
    dot = functools.partial(jnp.dot, preferred_element_type=jnp.float32)
    both = dot(jnp.concatenate([high, low], axis=0), table[0])
    return both[:rows] + both[rows:] + dot(high, table[1])


def partners(me, count):
    if count & (count - 1):
        return [lax.rem(me + step, count) for step in range(count)]
    peers, bit = [me], 1
    while bit < count:
        turn = bit * (1 - 2 * lax.rem(lax.div(me, bit), 2))
        peers += [peer + turn for peer in peers]
        bit *= 2
    return peers


def kernel(
    n_ya, n_zb, bounds,
    source, table_x, table_y, table_z, symbol_x, symbol_y, symbol_z,
    out, last, scale, tz,
    src, tx, ty, sx, sy, sz, first, second, third, lines, relay, column_x, base,
    local_sem, here_a, here_b, recv_a, recv_r, recv_b,
):
    ya, zb = lax.axis_index("ya"), lax.axis_index("zb")
    nx, yl, zl = source.shape
    ny = yl * n_ya
    kl = nx // n_ya
    jl = ny // n_zb
    chunks = len(bounds) - 1
    cuts = [0, *(c for c in CUTS if c < yl), yl]
    to_a, to_b = partners(ya, n_ya), partners(zb, n_zb)

    half, quarter = n_ya // 2, 0 if n_ya & (n_ya - 1) else n_ya // 4
    cross = [step ^ (quarter > 1) for step in range(half, n_ya)]
    aside = [*range(half - 1, 0, -1)]
    if not quarter:
        cross, aside = [*range(1, n_ya)], []
    lower_end, upper_end = ya < quarter, ya >= n_ya - quarter
    at_end = lower_end | upper_end
    inner = jnp.logical_not(at_end)
    nearby = to_a[quarter]

    barrier = pltpu.get_barrier_semaphore()

    def greet(axis, low, high):
        def one(peer, _):
            pl.semaphore_signal(barrier, inc=1, device_id={axis: peer}, device_id_type=MESH)
            return 0

        lax.fori_loop(low, high, one, 0)

    greet("ya", ya + 1, n_ya)
    greet("zb", zb + 1, n_zb)

    parts = len(cuts) - 1
    rows = [pl.ds(low, high - low) for low, high in zip(cuts, cuts[1:])]
    loads = [
        pltpu.make_async_copy(source.at[:, row], src.at[:, row], local_sem.at[i])
        for i, row in enumerate(rows)
    ]
    table = pltpu.make_async_copy(table_x, tx, local_sem.at[parts])
    send_a, send_r, send_b = [local_sem.at[i] for i in (parts + 1, 0, parts)]
    late = [
        pltpu.make_async_copy(a, b, local_sem.at[parts if i == 0 else i - 1 if i <= parts else i + 1])
        for i, (a, b) in enumerate(
            [(table_y, ty), (table_z, tz), (symbol_x, sx), (symbol_y, sy), (symbol_z, sz)]
        )
    ]
    table.start()
    for load in loads:
        load.start()

    flat_src = src.reshape(nx * yl, zl)
    flat_first = first.reshape(nx * yl, zl)

    def x_step(pair, _):
        values = jnp.concatenate(
            [flat_src[pl.ds(2 * pair + t, nx, stride=yl), :] for t in range(2)], axis=1
        )
        modes = left_product(tx[...], values)
        for t in range(2):
            flat_first[pl.ds(2 * pair + t, nx, stride=yl), :] = modes[:, t * zl:(t + 1) * zl]
        return 0

    def size(chunk):
        return bounds[chunk + 1] - bounds[chunk]

    def span(chunk):
        return pl.ds(bounds[chunk], size(chunk))

    def rows_of(peer, low, count):
        return pl.ds(pl.multiple_of(peer * yl + low, math.gcd(yl, low)), count)

    def copy_a(chunk, peer, low=0, count=yl):
        return pltpu.make_async_remote_copy(
            src_ref=first.at[peer, span(chunk), pl.ds(low, count)],
            dst_ref=second.at[span(chunk), rows_of(ya, low, count)],
            send_sem=send_a,
            recv_sem=recv_a.at[chunk],
            device_id={"ya": peer},
            device_id_type=MESH,
        )

    def hand_over(chunk, low=0, count=yl):
        other = jnp.where(ya < half, half, 0)
        return pltpu.make_async_remote_copy(
            src_ref=first.at[pl.ds(other, half), span(chunk), pl.ds(low, count)],
            dst_ref=relay.at[:, span(chunk), pl.ds(low, count)],
            send_sem=send_a,
            recv_sem=recv_r.at[chunk],
            device_id={"ya": nearby},
            device_id_type=MESH,
        )

    def pass_on(chunk, step):
        peer = to_a[step]
        return pltpu.make_async_remote_copy(
            src_ref=relay.at[lax.rem(peer, half), span(chunk)],
            dst_ref=second.at[span(chunk), rows_of(nearby, 0, yl)],
            send_sem=send_r,
            recv_sem=recv_a.at[chunk],
            device_id={"ya": peer},
            device_id_type=MESH,
        )

    def each_a(todo, lower, steps):
        for step in steps:
            peer = to_a[step]
            pl.when(peer < ya if lower else peer > ya)(functools.partial(todo, peer))

    def serve(chunk, peer, low=0, count=yl):
        copy_a(chunk, peer, low, count).start()

    def copy_b(chunk, step):
        peer = to_b[step]
        return pltpu.make_async_remote_copy(
            src_ref=third.at[span(chunk), pl.ds(pl.multiple_of(peer * jl, jl), jl)],
            dst_ref=last.at[zb] if chunk == chunks - 1 else lines.at[zb, span(chunk)],
            send_sem=send_b,
            recv_sem=recv_b.at[chunk],
            device_id={"zb": peer},
            device_id_type=MESH,
        )

    def all_of(ref, sem):
        return pltpu.make_async_copy(ref, ref, sem)

    def meet():
        below = ya + zb
        pl.when(below > 0)(lambda: pl.semaphore_wait(barrier, below))

        def answer(peer, _):
            pl.semaphore_signal(
                here_a.at[ya - 1], inc=1, device_id={"ya": peer}, device_id_type=MESH
            )
            return 0

        def answer_b(peer, _):
            pl.semaphore_signal(here_b, inc=1, device_id={"zb": peer}, device_id_type=MESH)
            return 0

        lax.fori_loop(jnp.where(ya < half, 0, quarter), ya, answer, 0)
        lax.fori_loop(0, zb, answer_b, 0)

    if BARPOS == 0:
        meet()
    for part in range(parts):
        low, count = cuts[part], cuts[part + 1] - cuts[part]
        if part == 0:
            table.wait()
            loads[0].wait()
            for i, load in enumerate(late):
                if i < 2 or i > parts:
                    load.start()
        else:
            loads[part].wait()
            if 2 <= part + 1 < len(late):
                late[part + 1].start()
        if part == 0 and BARPOS == 1:
            meet()
        lax.fori_loop(low // 2, (low + count) // 2, x_step, 0, unroll=True)
        if part == 0 and BARPOS == 2:
            meet()
        if quarter and not DIRECT:
            pl.when(upper_end)(lambda: hand_over(0, low, count).start())
        pl.when(inner | (upper_end & (DIRECT > 0)))(
            lambda: each_a(lambda peer: serve(0, peer, low, count), True, cross)
        )
        each_a(lambda peer: serve(0, peer, low, count), True, aside)

    near = [step for step in aside if step >= quarter] if quarter else []
    own = [step for step in aside if step not in near]

    if quarter:
        @pl.when(upper_end)
        def _():
            for turn in range(1, chunks + BEHIND):
                if turn < DIRECT:
                    each_a(functools.partial(serve, turn), True, cross)
                elif turn < chunks:
                    hand_over(turn).start()
                if turn < chunks:
                    each_a(functools.partial(serve, turn), True, own)
                if turn > BEHIND:
                    each_a(functools.partial(serve, turn - BEHIND), True, near)

        @pl.when(lower_end)
        def _():
            for chunk in range(1, chunks):
                each_a(functools.partial(serve, chunk), True, own)

    @pl.when(inner)
    def _():
        for chunk in range(1, chunks):
            if chunk < EARLY:
                each_a(functools.partial(serve, chunk), True, cross)
            each_a(functools.partial(serve, chunk), True, aside)

    for peer in range(1, n_ya):
        reached = peer > ya
        if quarter and peer >= half:
            reached &= jnp.logical_not(lower_end)

        @pl.when(reached)
        def _():
            pl.semaphore_wait(here_a.at[peer - 1], 1)
            if quarter:
                pl.when(lower_end & (nearby == peer))(lambda: hand_over(0).start())
            for chunk in range(min(EARLY, chunks)):
                serve(chunk, peer)

    if quarter:
        @pl.when(lower_end)
        def _():
            for turn in range(1, chunks + BEHIND):
                if turn < chunks:
                    hand_over(turn).start()
                if turn < chunks and turn >= EARLY:
                    each_a(functools.partial(serve, turn), False, own)
                if turn - BEHIND >= EARLY:
                    each_a(functools.partial(serve, turn - BEHIND), False, near)

        @pl.when(upper_end)
        def _():
            for chunk in range(EARLY, chunks):
                each_a(functools.partial(serve, chunk), False, own)

    @pl.when(inner)
    def _():
        for chunk in range(EARLY, chunks):
            each_a(functools.partial(serve, chunk), False, aside)

    second[:, pl.ds(pl.multiple_of(ya * yl, yl), yl), :] = first[ya]

    for load in late:
        load.wait()

    def column(row):
        return jnp.broadcast_to(row, (zl, row.shape[1])).T

    column_x[...] = column(sx[...])
    third[0] = column(sy[...])
    own_y = third[0, pl.ds(pl.multiple_of(zb * jl, jl), jl), :]
    base[...] = jnp.concatenate([own_y] * n_zb, axis=1) + sz[...]
    above = n_zb - 1 - zb
    pl.when(above > 0)(lambda: pl.semaphore_wait(here_b, above))

    def y_stage(chunk):
        all_of(second.at[span(chunk), pl.ds(0, ny - yl)], recv_a.at[chunk]).wait()
        for low in range(bounds[chunk], bounds[chunk + 1], 2):
            planes = range(low, min(low + 2, bounds[chunk + 1]))
            values = jnp.concatenate([second[k] for k in planes], axis=1)
            modes = left_product(ty[...], values)
            for t, k in enumerate(planes):
                third[k] = modes[:, t * zl:(t + 1) * zl]
        for step in range(n_zb - 1, 0, -1):
            copy_b(chunk, step).start()
        mine = third[span(chunk), pl.ds(pl.multiple_of(zb * jl, jl), jl), :]
        if chunk == chunks - 1:
            last[zb] = mine
        else:
            lines[zb, span(chunk)] = mine

    def scale_of(k):
        own_x = jnp.concatenate([column_x[pl.ds(ya * kl + k, 1), :]] * n_zb, axis=1)
        return lax.rsqrt(base[...] + own_x)

    for t in range(size(chunks - 1)):
        scale[t] = scale_of(bounds[-2] + t)

    def z_stage(chunk):
        all_of(third.at[span(chunk), pl.ds(0, ny - jl)], recv_b.at[chunk]).wait()
        if chunk == chunks - 1:
            return
        modes = right_product(lines, span(chunk), tz)
        for t in range(size(chunk)):
            k = bounds[chunk] + t
            out[k] = modes[t * jl:(t + 1) * jl] * scale_of(k)

    def push(turn):
        if quarter:
            got = all_of(relay.at[:, span(turn)], recv_r.at[turn])

            @pl.when(ya < half)
            def _():
                got.wait()
                for step in cross:
                    pass_on(turn, step).start()

            if turn >= DIRECT:
                @pl.when(ya >= half)
                def _():
                    got.wait()
                    for step in cross:
                        pl.when(to_a[step] == 0)(lambda: pass_on(turn, step).start())
                    rest = [
                        c for c in range(DIRECT, chunks)
                        if min(c + LEAD * (c >= LATE), chunks - 1) == turn
                    ]
                    for late in rest:
                        for step in cross:
                            pl.when(to_a[step] > 0)(lambda: pass_on(late, step).start())

        if turn + EARLY < chunks:
            for step in cross:
                serve(turn + EARLY, to_a[step])

    pushed = 0
    for turn in range(chunks + LAG):
        upto = min(chunks, 1 + BEYOND[turn] if turn < len(BEYOND) else chunks)
        if pushed < upto:
            @pl.when(inner)
            def _():
                for early in range(pushed, upto):
                    push(early)
            pushed = upto
        if turn < chunks:
            y_stage(turn)
        if turn >= LAG:
            z_stage(turn - LAG)

    all_of(first.at[pl.ds(0, n_ya - 1)], send_a).wait()
    if quarter:
        pl.when(inner & (ya < half))(lambda: all_of(relay, send_r).wait())
        later = relay.at[:, pl.ds(bounds[DIRECT], kl - bounds[DIRECT])]
        pl.when(inner & (ya >= half))(lambda: all_of(later, send_r).wait())
    all_of(third.at[:, pl.ds(0, ny - jl)], send_b).wait()


def finish(done, last, scale, table, out, final, sems):
    planes, rows = scale.shape[0], scale.shape[1]
    ready = done.shape[0] - planes
    cuts = [ready * piece // PIECES for piece in range(PIECES + 1)]
    copies = [
        pltpu.make_async_copy(done.at[low:high], out.at[low:high], sems.at[i])
        for i, (low, high) in enumerate(zip(cuts, cuts[1:]))
    ]
    for copy in copies:
        copy.start()
    modes = right_product(last, slice(None), table)
    for t in range(planes):
        final[t] = modes[t * rows:(t + 1) * rows] * scale[t]
        copies.append(pltpu.make_async_copy(final.at[t], out.at[ready + t], sems.at[PIECES + t]))
        copies[-1].start()
    for copy in copies:
        copy.wait()


def body(n_ya, n_zb, source, symbol_x, symbol_y, symbol_z):
    nx, yl, zl = source.shape
    ny, nz = yl * n_ya, zl * n_zb
    kl, jl = nx // n_ya, ny // n_zb
    ends = np.cumsum(SHARES) * kl // sum(SHARES)
    bounds = tuple(sorted({0, *ends.tolist()}))
    chunks = len(bounds) - 1
    tables = []
    for count in (nx, ny):
        high, low = transform_table(count)
        tables.append(np.concatenate([high, high, low], axis=1))
    tables.append(np.stack(transform_table(nz)))
    final = kl - bounds[-2]
    shapes = [(kl, jl, nz), (n_zb, final, jl, zl), (final, jl, nz)]
    room = 67_043_328 - 4 * sum(int(np.prod(shape)) for shape in shapes) - 4 * nz * nz - 2**18
    outs = [pltpu.VMEM(shape, jnp.float32) for shape in shapes]
    outs.append(pltpu.VMEM((2, nz, nz), jnp.bfloat16))
    dma = pltpu.SemaphoreType.DMA
    regular = pltpu.SemaphoreType.REGULAR
    vmem = pltpu.VMEM
    ready = pl.pallas_call(
        functools.partial(kernel, n_ya, n_zb, bounds),
        out_shape=outs,
        in_specs=[pl.BlockSpec(memory_space=pltpu.HBM)] * 7,
        out_specs=[pl.BlockSpec(memory_space=pltpu.VMEM)] * 4,
        scratch_shapes=[
            vmem((nx, yl, zl), jnp.float32),
            vmem((nx, 3 * nx), jnp.bfloat16),
            vmem((ny, 3 * ny), jnp.bfloat16),
            vmem((1, nx), jnp.float32),
            vmem((1, ny), jnp.float32),
            vmem((1, nz), jnp.float32),
            vmem((n_ya, kl, yl, zl), jnp.float32),
            vmem((kl, ny, zl), jnp.float32),
            vmem((kl, ny, zl), jnp.float32),
            vmem((n_zb, kl, jl, zl), jnp.float32),
            vmem((max(1, n_ya // 2), kl, yl, zl), jnp.float32),
            vmem((nx, zl), jnp.float32),
            vmem((jl, nz), jnp.float32),
            dma((2 + max(1 + sum(c < yl for c in CUTS), 4),)),
            regular((max(1, n_ya - 1),)),
            regular,
            dma((chunks,)),
            dma((chunks,)),
            dma((chunks,)),
        ],
        compiler_params=pltpu.CompilerParams(
            collective_id=0, has_side_effects=True, vmem_limit_bytes=room
        ),
    )(
        source, *[jnp.asarray(t) for t in tables],
        symbol_x[None], symbol_y[None], symbol_z[None],
    )
    return pl.pallas_call(
        finish,
        out_shape=jax.ShapeDtypeStruct((kl, jl, nz), jnp.float32),
        in_specs=[pl.BlockSpec(memory_space=pltpu.VMEM)] * 4,
        out_specs=pl.BlockSpec(memory_space=pltpu.HBM),
        scratch_shapes=[vmem((final, jl, nz), jnp.float32), dma((PIECES + final,))],
        compiler_params=pltpu.CompilerParams(vmem_limit_bytes=2**24),
    )(*[pltpu.with_memory_space_constraint(r, pltpu.VMEM) for r in ready])


def solution(mesh):
    placed = (P(None, "ya", "zb"), P(), P(), P())
    return jax.shard_map(
        functools.partial(body, mesh.shape["ya"], mesh.shape["zb"]),
        mesh=mesh, in_specs=placed, out_specs=P("ya", "zb", None), check_vma=False,
    )
```

```python
import functools
import math

import jax
import jax.numpy as jnp
import numpy as np
from jax import lax
from jax.experimental import pallas as pl
from jax.experimental.pallas import tpu as pltpu
from jax.sharding import PartitionSpec as P

MESH = pl.DeviceIdType.MESH
SHARES = (3, 3, 2, 2, 2, 2, 2)
LAG = 3
PIECES = 4
LEAD = 1
LATE = 2
BEHIND = 2
DIRECT = 2
CUTS = (2, 8)
BARPOS = 0
EARLY = 3
OFF = 1
SPLIT = 5
SHIFT = 0
BEYOND = (2, 4, 6)


def transform_table(count):
    rank = np.arange(1, count + 1)
    angle = np.pi / (count + 1) * (rank[:, None] * rank[None, :] % (2 * count + 2))
    table = np.sqrt(2.0 / (count + 1)) * np.sin(angle)
    high = table.astype(jnp.bfloat16)
    low = (table - high.astype(np.float64)).astype(jnp.bfloat16)
    return high, low


def halves(values):
    high = values.astype(jnp.bfloat16)
    return high, (values - high.astype(jnp.float32)).astype(jnp.bfloat16)


def left_product(table3, values):
    high, low = halves(values)
    stacked = jnp.concatenate([high, low, high], axis=0)
    return jnp.dot(table3, stacked, preferred_element_type=jnp.float32)


def right_product(lines, planes, table):
    parts = [lines[b, planes] for b in range(lines.shape[0])]
    rows = parts[0].shape[0] * parts[0].shape[1]
    values = jnp.concatenate([part.reshape(rows, part.shape[2]) for part in parts], axis=1)
    high, low = halves(values)
    dot = functools.partial(jnp.dot, preferred_element_type=jnp.float32)
    both = dot(jnp.concatenate([high, low], axis=0), table[0])
    return both[:rows] + both[rows:] + dot(high, table[1])


def partners(me, count):
    if count & (count - 1):
        return [lax.rem(me + step, count) for step in range(count)]
    peers, bit = [me], 1
    while bit < count:
        turn = bit * (1 - 2 * lax.rem(lax.div(me, bit), 2))
        peers += [peer + turn for peer in peers]
        bit *= 2
    return peers


def kernel(
    n_ya, n_zb, bounds,
    source, table_x, table_y, table_z, symbol_x, symbol_y, symbol_z,
    out, last, scale, tz,
    src, tx, ty, sx, sy, sz, first, second, third, lines, relay, column_x, base,
    local_sem, here_a, here_b, recv_a, recv_r, recv_b,
):
    ya, zb = lax.axis_index("ya"), lax.axis_index("zb")
    nx, yl, zl = source.shape
    ny = yl * n_ya
    kl = nx // n_ya
    jl = ny // n_zb
    chunks = len(bounds) - 1
    cuts = [0, *(c for c in CUTS if c < yl), yl]
    to_a, to_b = partners(ya, n_ya), partners(zb, n_zb)

    half, quarter = n_ya // 2, 0 if n_ya & (n_ya - 1) else n_ya // 4
    cross = [step ^ (quarter > 1) for step in range(half, n_ya)]
    aside = [*range(half - 1, 0, -1)]
    if not quarter:
        cross, aside = [*range(1, n_ya)], []
    lower_end, upper_end = ya < quarter, ya >= n_ya - quarter
    at_end = lower_end | upper_end
    inner = jnp.logical_not(at_end)
    nearby = to_a[quarter]

    barrier = pltpu.get_barrier_semaphore()

    def greet(axis, low, high):
        def one(peer, _):
            pl.semaphore_signal(barrier, inc=1, device_id={axis: peer}, device_id_type=MESH)
            return 0

        lax.fori_loop(low, high, one, 0)

    greet("ya", ya + 1, n_ya)
    greet("zb", zb + 1, n_zb)

    parts = len(cuts) - 1
    rows = [pl.ds(low, high - low) for low, high in zip(cuts, cuts[1:])]
    loads = [
        pltpu.make_async_copy(source.at[:, row], src.at[:, row], local_sem.at[i])
        for i, row in enumerate(rows)
    ]
    table = pltpu.make_async_copy(table_x, tx, local_sem.at[parts])
    send_a, send_r, send_b = [local_sem.at[i] for i in (parts + 1, 0, parts)]
    late = [
        pltpu.make_async_copy(a, b, local_sem.at[parts if i == 0 else i - 1 if i <= parts else i + 1])
        for i, (a, b) in enumerate(
            [(table_y, ty), (table_z, tz), (symbol_x, sx), (symbol_y, sy), (symbol_z, sz)]
        )
    ]
    table.start()
    for load in loads:
        load.start()

    flat_src = src.reshape(nx * yl, zl)
    flat_first = first.reshape(nx * yl, zl)

    def x_step(pair, _):
        values = jnp.concatenate(
            [flat_src[pl.ds(2 * pair + t, nx, stride=yl), :] for t in range(2)], axis=1
        )
        modes = left_product(tx[...], values)
        for t in range(2):
            flat_first[pl.ds(2 * pair + t, nx, stride=yl), :] = modes[:, t * zl:(t + 1) * zl]
        return 0

    def size(chunk):
        return bounds[chunk + 1] - bounds[chunk]

    def span(chunk):
        return pl.ds(bounds[chunk], size(chunk))

    def rows_of(peer, low, count):
        return pl.ds(pl.multiple_of(peer * yl + low, math.gcd(yl, low)), count)

    def copy_a(chunk, peer, low=0, count=yl):
        return pltpu.make_async_remote_copy(
            src_ref=first.at[peer, span(chunk), pl.ds(low, count)],
            dst_ref=second.at[span(chunk), rows_of(ya, low, count)],
            send_sem=send_a,
            recv_sem=recv_a.at[chunk],
            device_id={"ya": peer},
            device_id_type=MESH,
        )

    def hand_over(chunk, low=0, count=yl):
        other = jnp.where(ya < half, half, 0)
        return pltpu.make_async_remote_copy(
            src_ref=first.at[pl.ds(other, half), span(chunk), pl.ds(low, count)],
            dst_ref=relay.at[:, span(chunk), pl.ds(low, count)],
            send_sem=send_a,
            recv_sem=recv_r.at[chunk],
            device_id={"ya": nearby},
            device_id_type=MESH,
        )

    def pass_on(chunk, step):
        peer = to_a[step]
        return pltpu.make_async_remote_copy(
            src_ref=relay.at[lax.rem(peer, half), span(chunk)],
            dst_ref=second.at[span(chunk), rows_of(nearby, 0, yl)],
            send_sem=send_r,
            recv_sem=recv_a.at[chunk],
            device_id={"ya": peer},
            device_id_type=MESH,
        )

    def each_a(todo, lower, steps):
        for step in steps:
            peer = to_a[step]
            pl.when(peer < ya if lower else peer > ya)(functools.partial(todo, peer))

    def serve(chunk, peer, low=0, count=yl):
        copy_a(chunk, peer, low, count).start()

    def copy_b(chunk, step):
        peer = to_b[step]
        return pltpu.make_async_remote_copy(
            src_ref=third.at[span(chunk), pl.ds(pl.multiple_of(peer * jl, jl), jl)],
            dst_ref=last.at[zb] if chunk == chunks - 1 else lines.at[zb, span(chunk)],
            send_sem=send_b,
            recv_sem=recv_b.at[chunk],
            device_id={"zb": peer},
            device_id_type=MESH,
        )

    def all_of(ref, sem):
        return pltpu.make_async_copy(ref, ref, sem)

    def meet():
        below = ya + zb
        pl.when(below > 0)(lambda: pl.semaphore_wait(barrier, below))

        def answer(peer, _):
            pl.semaphore_signal(
                here_a.at[ya - 1], inc=1, device_id={"ya": peer}, device_id_type=MESH
            )
            return 0

        def answer_b(peer, _):
            pl.semaphore_signal(here_b, inc=1, device_id={"zb": peer}, device_id_type=MESH)
            return 0

        lax.fori_loop(jnp.where(ya < half, 0, quarter), ya, answer, 0)
        lax.fori_loop(0, zb, answer_b, 0)

    if BARPOS == 0:
        meet()
    for part in range(parts):
        low, count = cuts[part], cuts[part + 1] - cuts[part]
        if part == 0:
            table.wait()
            loads[0].wait()
            for i, load in enumerate(late):
                if i < 2 or i > parts:
                    load.start()
        else:
            loads[part].wait()
            if 2 <= part + 1 < len(late):
                late[part + 1].start()
        if part == 0 and BARPOS == 1:
            meet()
        lax.fori_loop(low // 2, (low + count) // 2, x_step, 0, unroll=True)
        if part == 0 and BARPOS == 2:
            meet()
        if quarter and not DIRECT:
            pl.when(upper_end)(lambda: hand_over(0, low, count).start())
        pl.when(inner | (upper_end & (DIRECT > 0)))(
            lambda: each_a(lambda peer: serve(0, peer, low, count), True, cross)
        )
        each_a(lambda peer: serve(0, peer, low, count), True, aside)

    near = [step for step in aside if step >= quarter] if quarter else []
    own = [step for step in aside if step not in near]

    if quarter:
        @pl.when(upper_end)
        def _():
            for turn in range(1, chunks + BEHIND):
                if turn < DIRECT:
                    each_a(functools.partial(serve, turn), True, cross)
                elif turn < chunks:
                    hand_over(turn).start()
                if turn < chunks:
                    each_a(functools.partial(serve, turn), True, own)
                if turn > BEHIND:
                    each_a(functools.partial(serve, turn - BEHIND), True, near)

        @pl.when(lower_end)
        def _():
            for chunk in range(1, chunks):
                each_a(functools.partial(serve, chunk), True, own)

    @pl.when(inner)
    def _():
        for chunk in range(1, chunks):
            if chunk < EARLY:
                each_a(functools.partial(serve, chunk), True, cross)
            each_a(functools.partial(serve, chunk), True, aside)

    for peer in range(1, n_ya):
        reached = peer > ya
        if quarter and peer >= half:
            reached &= jnp.logical_not(lower_end)

        @pl.when(reached)
        def _():
            pl.semaphore_wait(here_a.at[peer - 1], 1)
            if quarter:
                pl.when(lower_end & (nearby == peer))(lambda: hand_over(0).start())
            for chunk in range(min(EARLY, chunks)):
                serve(chunk, peer)

    if quarter:
        @pl.when(lower_end)
        def _():
            for turn in range(1, chunks + BEHIND):
                if turn < chunks:
                    hand_over(turn).start()
                if turn < chunks and turn >= EARLY:
                    each_a(functools.partial(serve, turn), False, own)
                if turn - BEHIND >= EARLY:
                    each_a(functools.partial(serve, turn - BEHIND), False, near)

        @pl.when(upper_end)
        def _():
            for chunk in range(EARLY, chunks):
                each_a(functools.partial(serve, chunk), False, own)

    @pl.when(inner)
    def _():
        for chunk in range(EARLY, chunks):
            each_a(functools.partial(serve, chunk), False, aside)

    second[:, pl.ds(pl.multiple_of(ya * yl, yl), yl), :] = first[ya]

    for load in late:
        load.wait()

    def column(row):
        return jnp.broadcast_to(row, (zl, row.shape[1])).T

    column_x[...] = column(sx[...])
    third[0] = column(sy[...])
    own_y = third[0, pl.ds(pl.multiple_of(zb * jl, jl), jl), :]
    base[...] = jnp.concatenate([own_y] * n_zb, axis=1) + sz[...]
    above = n_zb - 1 - zb
    pl.when(above > 0)(lambda: pl.semaphore_wait(here_b, above))

    def y_stage(chunk):
        all_of(second.at[span(chunk), pl.ds(0, ny - yl)], recv_a.at[chunk]).wait()
        for low in range(bounds[chunk], bounds[chunk + 1], 2):
            planes = range(low, min(low + 2, bounds[chunk + 1]))
            values = jnp.concatenate([second[k] for k in planes], axis=1)
            modes = left_product(ty[...], values)
            for t, k in enumerate(planes):
                third[k] = modes[:, t * zl:(t + 1) * zl]
        for step in range(n_zb - 1, 0, -1):
            copy_b(chunk, step).start()
        mine = third[span(chunk), pl.ds(pl.multiple_of(zb * jl, jl), jl), :]
        if chunk == chunks - 1:
            last[zb] = mine
        else:
            lines[zb, span(chunk)] = mine

    def scale_of(k):
        own_x = jnp.concatenate([column_x[pl.ds(ya * kl + k, 1), :]] * n_zb, axis=1)
        return lax.rsqrt(base[...] + own_x)

    for t in range(size(chunks - 1)):
        scale[t] = scale_of(bounds[-2] + t)

    def z_stage(chunk):
        all_of(third.at[span(chunk), pl.ds(0, ny - jl)], recv_b.at[chunk]).wait()
        if chunk == chunks - 1:
            return
        modes = right_product(lines, span(chunk), tz)
        for t in range(size(chunk)):
            k = bounds[chunk] + t
            out[k] = modes[t * jl:(t + 1) * jl] * scale_of(k)

    def push(turn):
        own_due = turn + OFF if EARLY <= turn + OFF < chunks else None

        def own(chunk, wanted):
            for step in cross:
                peer = to_a[step]
                pl.when(wanted(peer))(functools.partial(serve, chunk, peer))

        def passed(chunk, wanted):
            for step in cross:
                pl.when(wanted(to_a[step]))(lambda: pass_on(chunk, step).start())

        def anyone(peer):
            return peer >= 0

        def first_one(peer):
            return peer == 0

        def the_rest(peer):
            return peer > 0

        got = all_of(relay.at[:, span(turn)], recv_r.at[turn]) if quarter else None

        @pl.when(ya < half)
        def _():
            if quarter:
                got.wait()
                passed(turn, anyone)
            if own_due is not None:
                own(own_due, anyone)

        @pl.when(ya >= half)
        def _():
            if quarter and turn >= DIRECT:
                got.wait()
                passed(turn, first_one)
            if own_due is not None:
                own(own_due, first_one)
            rest = [(c, True) for c in range(EARLY, chunks) if c >= SPLIT and c == turn + SHIFT]
            if own_due is not None and own_due < SPLIT:
                rest.append((own_due, True))
            for c in range(DIRECT, chunks) if quarter else ():
                if min(c + LEAD * (c >= LATE), chunks - 1) == turn:
                    rest.append((c, False))
            for c, mine in rest:
                (own if mine else passed)(c, the_rest)

    pushed = 0
    for turn in range(chunks + LAG):
        upto = min(chunks, 1 + BEYOND[turn] if turn < len(BEYOND) else chunks)
        if pushed < upto:
            @pl.when(inner)
            def _():
                for early in range(pushed, upto):
                    push(early)
            pushed = upto
        if turn < chunks:
            y_stage(turn)
        if turn >= LAG:
            z_stage(turn - LAG)

    all_of(first.at[pl.ds(0, n_ya - 1)], send_a).wait()
    if quarter:
        pl.when(inner & (ya < half))(lambda: all_of(relay, send_r).wait())
        later = relay.at[:, pl.ds(bounds[DIRECT], kl - bounds[DIRECT])]
        pl.when(inner & (ya >= half))(lambda: all_of(later, send_r).wait())
    all_of(third.at[:, pl.ds(0, ny - jl)], send_b).wait()


def finish(done, last, scale, table, out, final, sems):
    planes, rows = scale.shape[0], scale.shape[1]
    ready = done.shape[0] - planes
    cuts = [ready * piece // PIECES for piece in range(PIECES + 1)]
    copies = [
        pltpu.make_async_copy(done.at[low:high], out.at[low:high], sems.at[i])
        for i, (low, high) in enumerate(zip(cuts, cuts[1:]))
    ]
    for copy in copies:
        copy.start()
    modes = right_product(last, slice(None), table)
    for t in range(planes):
        final[t] = modes[t * rows:(t + 1) * rows] * scale[t]
        copies.append(pltpu.make_async_copy(final.at[t], out.at[ready + t], sems.at[PIECES + t]))
        copies[-1].start()
    for copy in copies:
        copy.wait()


def body(n_ya, n_zb, source, symbol_x, symbol_y, symbol_z):
    nx, yl, zl = source.shape
    ny, nz = yl * n_ya, zl * n_zb
    kl, jl = nx // n_ya, ny // n_zb
    ends = np.cumsum(SHARES) * kl // sum(SHARES)
    bounds = tuple(sorted({0, *ends.tolist()}))
    chunks = len(bounds) - 1
    tables = []
    for count in (nx, ny):
        high, low = transform_table(count)
        tables.append(np.concatenate([high, high, low], axis=1))
    tables.append(np.stack(transform_table(nz)))
    final = kl - bounds[-2]
    shapes = [(kl, jl, nz), (n_zb, final, jl, zl), (final, jl, nz)]
    room = 67_043_328 - 4 * sum(int(np.prod(shape)) for shape in shapes) - 4 * nz * nz - 2**18
    outs = [pltpu.VMEM(shape, jnp.float32) for shape in shapes]
    outs.append(pltpu.VMEM((2, nz, nz), jnp.bfloat16))
    dma = pltpu.SemaphoreType.DMA
    regular = pltpu.SemaphoreType.REGULAR
    vmem = pltpu.VMEM
    ready = pl.pallas_call(
        functools.partial(kernel, n_ya, n_zb, bounds),
        out_shape=outs,
        in_specs=[pl.BlockSpec(memory_space=pltpu.HBM)] * 7,
        out_specs=[pl.BlockSpec(memory_space=pltpu.VMEM)] * 4,
        scratch_shapes=[
            vmem((nx, yl, zl), jnp.float32),
            vmem((nx, 3 * nx), jnp.bfloat16),
            vmem((ny, 3 * ny), jnp.bfloat16),
            vmem((1, nx), jnp.float32),
            vmem((1, ny), jnp.float32),
            vmem((1, nz), jnp.float32),
            vmem((n_ya, kl, yl, zl), jnp.float32),
            vmem((kl, ny, zl), jnp.float32),
            vmem((kl, ny, zl), jnp.float32),
            vmem((n_zb, kl, jl, zl), jnp.float32),
            vmem((max(1, n_ya // 2), kl, yl, zl), jnp.float32),
            vmem((nx, zl), jnp.float32),
            vmem((jl, nz), jnp.float32),
            dma((2 + max(1 + sum(c < yl for c in CUTS), 4),)),
            regular((max(1, n_ya - 1),)),
            regular,
            dma((chunks,)),
            dma((chunks,)),
            dma((chunks,)),
        ],
        compiler_params=pltpu.CompilerParams(
            collective_id=0, has_side_effects=True, vmem_limit_bytes=room
        ),
    )(
        source, *[jnp.asarray(t) for t in tables],
        symbol_x[None], symbol_y[None], symbol_z[None],
    )
    return pl.pallas_call(
        finish,
        out_shape=jax.ShapeDtypeStruct((kl, jl, nz), jnp.float32),
        in_specs=[pl.BlockSpec(memory_space=pltpu.VMEM)] * 4,
        out_specs=pl.BlockSpec(memory_space=pltpu.HBM),
        scratch_shapes=[vmem((final, jl, nz), jnp.float32), dma((PIECES + final,))],
        compiler_params=pltpu.CompilerParams(vmem_limit_bytes=2**24),
    )(*[pltpu.with_memory_space_constraint(r, pltpu.VMEM) for r in ready])


def solution(mesh):
    placed = (P(None, "ya", "zb"), P(), P(), P())
    return jax.shard_map(
        functools.partial(body, mesh.shape["ya"], mesh.shape["zb"]),
        mesh=mesh, in_specs=placed, out_specs=P("ya", "zb", None), check_vma=False,
    )
```

```python
import functools
import math

import jax
import jax.numpy as jnp
import numpy as np
from jax import lax
from jax.experimental import pallas as pl
from jax.experimental.pallas import tpu as pltpu
from jax.sharding import PartitionSpec as P

MESH = pl.DeviceIdType.MESH
SHARES = (3, 3, 3, 3, 2, 1, 1)
LAG = 3
PIECES = 4
LEAD = 1
BEHIND = 2
DIRECT = 2
CUTS = (2, 8)
EARLY = 3
OFF = 1
SPLIT = 5
TAIL = 3
BEYOND = (2, 4, 5, 6)


def transform_table(count):
    rank = np.arange(1, count + 1)
    angle = np.pi / (count + 1) * (rank[:, None] * rank[None, :] % (2 * count + 2))
    table = np.sqrt(2.0 / (count + 1)) * np.sin(angle)
    high = table.astype(jnp.bfloat16)
    low = (table - high.astype(np.float64)).astype(jnp.bfloat16)
    return high, low


def halves(values):
    high = values.astype(jnp.bfloat16)
    return high, (values - high.astype(jnp.float32)).astype(jnp.bfloat16)


def left_product(table3, values):
    high, low = halves(values)
    stacked = jnp.concatenate([high, low, high], axis=0)
    return jnp.dot(table3, stacked, preferred_element_type=jnp.float32)


def right_product(lines, planes, table):
    parts = [lines[b, planes] for b in range(lines.shape[0])]
    rows = parts[0].shape[0] * parts[0].shape[1]
    values = jnp.concatenate([part.reshape(rows, part.shape[2]) for part in parts], axis=1)
    high, low = halves(values)
    dot = functools.partial(jnp.dot, preferred_element_type=jnp.float32)
    both = dot(jnp.concatenate([high, low], axis=0), table[0])
    return both[:rows] + both[rows:] + dot(high, table[1])


def partners(me, count):
    if count & (count - 1):
        return [lax.rem(me + step, count) for step in range(count)]
    peers, bit = [me], 1
    while bit < count:
        turn = bit * (1 - 2 * lax.rem(lax.div(me, bit), 2))
        peers += [peer + turn for peer in peers]
        bit *= 2
    return peers


def kernel(
    n_ya, n_zb, bounds,
    source, table_x, table_y, table_z, symbol_x, symbol_y, symbol_z,
    out, last, scale, tz,
    src, tx, ty, sx, sy, sz, first, second, third, lines, relay, column_x, base,
    local_sem, here_a, here_b, recv_a, recv_r, recv_b,
):
    ya, zb = lax.axis_index("ya"), lax.axis_index("zb")
    nx, yl, zl = source.shape
    ny = yl * n_ya
    kl = nx // n_ya
    jl = ny // n_zb
    chunks = len(bounds) - 1
    cuts = [0, *(c for c in CUTS if c < yl), yl]
    to_a, to_b = partners(ya, n_ya), partners(zb, n_zb)

    half, quarter = n_ya // 2, 0 if n_ya & (n_ya - 1) else n_ya // 4
    cross = [step ^ (quarter > 1) for step in range(half, n_ya)]
    aside = [*range(half - 1, 0, -1)]
    if not quarter:
        cross, aside = [*range(1, n_ya)], []
    lower_end, upper_end = ya < quarter, ya >= n_ya - quarter
    at_end = lower_end | upper_end
    inner = jnp.logical_not(at_end)
    nearby = to_a[quarter]

    barrier = pltpu.get_barrier_semaphore()

    def greet(axis, low, high):
        def one(peer, _):
            pl.semaphore_signal(barrier, inc=1, device_id={axis: peer}, device_id_type=MESH)
            return 0

        lax.fori_loop(low, high, one, 0)

    greet("ya", ya + 1, n_ya)
    greet("zb", zb + 1, n_zb)

    parts = len(cuts) - 1
    rows = [pl.ds(low, high - low) for low, high in zip(cuts, cuts[1:])]
    loads = [
        pltpu.make_async_copy(source.at[:, row], src.at[:, row], local_sem.at[i])
        for i, row in enumerate(rows)
    ]
    table = pltpu.make_async_copy(table_x, tx, local_sem.at[parts])
    send_a, send_r, send_b = [local_sem.at[i] for i in (parts + 1, 0, parts)]
    late = [
        pltpu.make_async_copy(a, b, local_sem.at[parts if i == 0 else i - 1 if i <= parts else i + 1])
        for i, (a, b) in enumerate(
            [(table_y, ty), (table_z, tz), (symbol_x, sx), (symbol_y, sy), (symbol_z, sz)]
        )
    ]
    table.start()
    for load in loads:
        load.start()

    flat_src = src.reshape(nx * yl, zl)
    flat_first = first.reshape(nx * yl, zl)

    def x_step(pair, _):
        values = jnp.concatenate(
            [flat_src[pl.ds(2 * pair + t, nx, stride=yl), :] for t in range(2)], axis=1
        )
        modes = left_product(tx[...], values)
        for t in range(2):
            flat_first[pl.ds(2 * pair + t, nx, stride=yl), :] = modes[:, t * zl:(t + 1) * zl]
        return 0

    def size(chunk):
        return bounds[chunk + 1] - bounds[chunk]

    def span(chunk):
        return pl.ds(bounds[chunk], size(chunk))

    def rows_of(peer, low, count):
        return pl.ds(pl.multiple_of(peer * yl + low, math.gcd(yl, low)), count)

    def copy_a(chunk, peer, low=0, count=yl):
        return pltpu.make_async_remote_copy(
            src_ref=first.at[peer, span(chunk), pl.ds(low, count)],
            dst_ref=second.at[span(chunk), rows_of(ya, low, count)],
            send_sem=send_a,
            recv_sem=recv_a.at[chunk],
            device_id={"ya": peer},
            device_id_type=MESH,
        )

    def hand_over(chunk, low=0, count=yl):
        other = jnp.where(ya < half, half, 0)
        return pltpu.make_async_remote_copy(
            src_ref=first.at[pl.ds(other, half), span(chunk), pl.ds(low, count)],
            dst_ref=relay.at[:, span(chunk), pl.ds(low, count)],
            send_sem=send_a,
            recv_sem=recv_r.at[chunk],
            device_id={"ya": nearby},
            device_id_type=MESH,
        )

    def pass_on(chunk, step):
        peer = to_a[step]
        return pltpu.make_async_remote_copy(
            src_ref=relay.at[lax.rem(peer, half), span(chunk)],
            dst_ref=second.at[span(chunk), rows_of(nearby, 0, yl)],
            send_sem=send_r,
            recv_sem=recv_a.at[chunk],
            device_id={"ya": peer},
            device_id_type=MESH,
        )

    def each_a(todo, lower, steps):
        for step in steps:
            peer = to_a[step]
            pl.when(peer < ya if lower else peer > ya)(functools.partial(todo, peer))

    def serve(chunk, peer, low=0, count=yl):
        copy_a(chunk, peer, low, count).start()

    def copy_b(chunk, step):
        peer = to_b[step]
        return pltpu.make_async_remote_copy(
            src_ref=third.at[span(chunk), pl.ds(pl.multiple_of(peer * jl, jl), jl)],
            dst_ref=last.at[zb] if chunk == chunks - 1 else lines.at[zb, span(chunk)],
            send_sem=send_b,
            recv_sem=recv_b.at[chunk],
            device_id={"zb": peer},
            device_id_type=MESH,
        )

    def all_of(ref, sem):
        return pltpu.make_async_copy(ref, ref, sem)

    def meet():
        below = ya + zb
        pl.when(below > 0)(lambda: pl.semaphore_wait(barrier, below))

        def answer(peer, _):
            pl.semaphore_signal(
                here_a.at[ya - 1], inc=1, device_id={"ya": peer}, device_id_type=MESH
            )
            return 0

        def answer_b(peer, _):
            pl.semaphore_signal(here_b, inc=1, device_id={"zb": peer}, device_id_type=MESH)
            return 0

        lax.fori_loop(jnp.where(ya < half, 0, quarter), ya, answer, 0)
        lax.fori_loop(0, zb, answer_b, 0)

    even = lax.rem(ya, 2) == 0
    pl.when(jnp.logical_not(even))(meet)
    for part in range(parts):
        low, count = cuts[part], cuts[part + 1] - cuts[part]
        if part == 0:
            table.wait()
            loads[0].wait()
            for i, load in enumerate(late):
                if i < 2 or i > parts:
                    load.start()
        else:
            loads[part].wait()
            if 2 <= part + 1 < len(late):
                late[part + 1].start()
        lax.fori_loop(low // 2, (low + count) // 2, x_step, 0, unroll=True)
        if part == 0:
            pl.when(even)(meet)
        if quarter and not DIRECT:
            pl.when(upper_end)(lambda: hand_over(0, low, count).start())
        pl.when(inner | (upper_end & (DIRECT > 0)))(
            lambda: each_a(lambda peer: serve(0, peer, low, count), True, cross)
        )
        each_a(lambda peer: serve(0, peer, low, count), True, aside)

    near = [step for step in aside if step >= quarter] if quarter else []
    own = [step for step in aside if step not in near]

    if quarter:
        @pl.when(upper_end)
        def _():
            for turn in range(1, chunks + BEHIND):
                if turn < DIRECT:
                    each_a(functools.partial(serve, turn), True, cross)
                elif turn < chunks:
                    hand_over(turn).start()
                if turn < chunks:
                    each_a(functools.partial(serve, turn), True, own)
                if turn > BEHIND:
                    each_a(functools.partial(serve, turn - BEHIND), True, near)

        @pl.when(lower_end)
        def _():
            for chunk in range(1, chunks):
                each_a(functools.partial(serve, chunk), True, own)

    @pl.when(inner)
    def _():
        for chunk in range(1, chunks):
            if chunk < EARLY:
                each_a(functools.partial(serve, chunk), True, cross)
            each_a(functools.partial(serve, chunk), True, aside)

    for peer in range(1, n_ya):
        reached = peer > ya
        if quarter and peer >= half:
            reached &= jnp.logical_not(lower_end)

        @pl.when(reached)
        def _():
            pl.semaphore_wait(here_a.at[peer - 1], 1)
            if quarter:
                pl.when(lower_end & (nearby == peer))(lambda: hand_over(0).start())
            for chunk in range(min(EARLY, chunks)):
                serve(chunk, peer)

    if quarter:
        @pl.when(lower_end)
        def _():
            for turn in range(1, chunks + BEHIND):
                if turn < chunks:
                    hand_over(turn).start()
                if turn < chunks and turn >= EARLY:
                    each_a(functools.partial(serve, turn), False, own)
                if turn - BEHIND >= EARLY:
                    each_a(functools.partial(serve, turn - BEHIND), False, near)

        @pl.when(upper_end)
        def _():
            for chunk in range(EARLY, chunks):
                each_a(functools.partial(serve, chunk), False, own)

    @pl.when(inner)
    def _():
        for chunk in range(EARLY, chunks):
            each_a(functools.partial(serve, chunk), False, aside)

    second[:, pl.ds(pl.multiple_of(ya * yl, yl), yl), :] = first[ya]

    for load in late:
        load.wait()

    def column(row):
        return jnp.broadcast_to(row, (zl, row.shape[1])).T

    column_x[...] = column(sx[...])
    third[0] = column(sy[...])
    own_y = third[0, pl.ds(pl.multiple_of(zb * jl, jl), jl), :]
    base[...] = jnp.concatenate([own_y] * n_zb, axis=1) + sz[...]
    above = n_zb - 1 - zb
    pl.when(above > 0)(lambda: pl.semaphore_wait(here_b, above))

    def y_stage(chunk):
        all_of(second.at[span(chunk), pl.ds(0, ny - yl)], recv_a.at[chunk]).wait()
        for low in range(bounds[chunk], bounds[chunk + 1], 2):
            planes = range(low, min(low + 2, bounds[chunk + 1]))
            values = jnp.concatenate([second[k] for k in planes], axis=1)
            modes = left_product(ty[...], values)
            for t, k in enumerate(planes):
                third[k] = modes[:, t * zl:(t + 1) * zl]
        for step in range(n_zb - 1, 0, -1):
            copy_b(chunk, step).start()
        mine = third[span(chunk), pl.ds(pl.multiple_of(zb * jl, jl), jl), :]
        if chunk == chunks - 1:
            last[zb] = mine
        else:
            lines[zb, span(chunk)] = mine

    def scale_of(k):
        own_x = jnp.concatenate([column_x[pl.ds(ya * kl + k, 1), :]] * n_zb, axis=1)
        return lax.rsqrt(base[...] + own_x)

    for t in range(size(chunks - 1)):
        scale[t] = scale_of(bounds[-2] + t)

    def z_stage(chunk):
        all_of(third.at[span(chunk), pl.ds(0, ny - jl)], recv_b.at[chunk]).wait()
        if chunk == chunks - 1:
            return
        modes = right_product(lines, span(chunk), tz)
        for t in range(size(chunk)):
            k = bounds[chunk] + t
            out[k] = modes[t * jl:(t + 1) * jl] * scale_of(k)

    def later(chunk, start, offset):
        if chunk >= chunks - TAIL:
            return chunks - 1
        if offset > 0:
            return chunk if chunk >= start else chunk - offset
        return min(chunk - offset, chunks - 1)

    def push(turn):
        own_due = turn + OFF if EARLY <= turn + OFF < chunks else None

        def own(chunk, wanted):
            for step in cross:
                peer = to_a[step]
                pl.when(wanted(peer))(functools.partial(serve, chunk, peer))

        def passed(chunk, wanted):
            for step in cross:
                pl.when(wanted(to_a[step]))(lambda: pass_on(chunk, step).start())

        def anyone(peer):
            return peer >= 0

        def first_one(peer):
            return peer == 0

        def the_rest(peer):
            return peer > 0

        got = all_of(relay.at[:, span(turn)], recv_r.at[turn]) if quarter else None

        @pl.when(ya < half)
        def _():
            if quarter:
                got.wait()
                passed(turn, anyone)
            if own_due is not None:
                own(own_due, anyone)

        @pl.when(ya >= half)
        def _():
            if quarter and turn >= DIRECT:
                got.wait()
                passed(turn, first_one)
            if own_due is not None:
                own(own_due, first_one)
            rest = [(c, 0) for c in range(EARLY, chunks) if later(c, SPLIT, OFF) == turn]
            if quarter:
                rest += [(c, 1) for c in range(DIRECT, chunks) if later(c, DIRECT, -LEAD) == turn]
            rest.sort()
            for c, relayed in rest:
                (passed if relayed else own)(c, the_rest)

    pushed = 0
    for turn in range(chunks + LAG):
        upto = min(chunks, 1 + BEYOND[turn] if turn < len(BEYOND) else chunks)
        if pushed < upto:
            @pl.when(inner)
            def _():
                for early in range(pushed, upto):
                    push(early)
            pushed = upto
        if turn < chunks:
            y_stage(turn)
        if turn >= LAG:
            z_stage(turn - LAG)

    all_of(first.at[pl.ds(0, n_ya - 1)], send_a).wait()
    if quarter:
        pl.when(inner & (ya < half))(lambda: all_of(relay, send_r).wait())
        later = relay.at[:, pl.ds(bounds[DIRECT], kl - bounds[DIRECT])]
        pl.when(inner & (ya >= half))(lambda: all_of(later, send_r).wait())
    all_of(third.at[:, pl.ds(0, ny - jl)], send_b).wait()


def finish(done, last, scale, table, out, final, sems):
    planes, rows = scale.shape[0], scale.shape[1]
    ready = done.shape[0] - planes
    cuts = [ready * piece // PIECES for piece in range(PIECES + 1)]
    copies = [
        pltpu.make_async_copy(done.at[low:high], out.at[low:high], sems.at[i])
        for i, (low, high) in enumerate(zip(cuts, cuts[1:]))
    ]
    for copy in copies:
        copy.start()
    modes = right_product(last, slice(None), table)
    for t in range(planes):
        final[t] = modes[t * rows:(t + 1) * rows] * scale[t]
        copies.append(pltpu.make_async_copy(final.at[t], out.at[ready + t], sems.at[PIECES + t]))
        copies[-1].start()
    for copy in copies:
        copy.wait()


def body(n_ya, n_zb, source, symbol_x, symbol_y, symbol_z):
    nx, yl, zl = source.shape
    ny, nz = yl * n_ya, zl * n_zb
    kl, jl = nx // n_ya, ny // n_zb
    ends = np.cumsum(SHARES) * kl // sum(SHARES)
    bounds = tuple(sorted({0, *ends.tolist()}))
    chunks = len(bounds) - 1
    tables = []
    for count in (nx, ny):
        high, low = transform_table(count)
        tables.append(np.concatenate([high, high, low], axis=1))
    tables.append(np.stack(transform_table(nz)))
    final = kl - bounds[-2]
    shapes = [(kl, jl, nz), (n_zb, final, jl, zl), (final, jl, nz)]
    room = 67_043_328 - 4 * sum(int(np.prod(shape)) for shape in shapes) - 4 * nz * nz - 2**18
    outs = [pltpu.VMEM(shape, jnp.float32) for shape in shapes]
    outs.append(pltpu.VMEM((2, nz, nz), jnp.bfloat16))
    dma = pltpu.SemaphoreType.DMA
    regular = pltpu.SemaphoreType.REGULAR
    vmem = pltpu.VMEM
    ready = pl.pallas_call(
        functools.partial(kernel, n_ya, n_zb, bounds),
        out_shape=outs,
        in_specs=[pl.BlockSpec(memory_space=pltpu.HBM)] * 7,
        out_specs=[pl.BlockSpec(memory_space=pltpu.VMEM)] * 4,
        scratch_shapes=[
            vmem((nx, yl, zl), jnp.float32),
            vmem((nx, 3 * nx), jnp.bfloat16),
            vmem((ny, 3 * ny), jnp.bfloat16),
            vmem((1, nx), jnp.float32),
            vmem((1, ny), jnp.float32),
            vmem((1, nz), jnp.float32),
            vmem((n_ya, kl, yl, zl), jnp.float32),
            vmem((kl, ny, zl), jnp.float32),
            vmem((kl, ny, zl), jnp.float32),
            vmem((n_zb, kl, jl, zl), jnp.float32),
            vmem((max(1, n_ya // 2), kl, yl, zl), jnp.float32),
            vmem((nx, zl), jnp.float32),
            vmem((jl, nz), jnp.float32),
            dma((2 + max(1 + sum(c < yl for c in CUTS), 4),)),
            regular((max(1, n_ya - 1),)),
            regular,
            dma((chunks,)),
            dma((chunks,)),
            dma((chunks,)),
        ],
        compiler_params=pltpu.CompilerParams(
            collective_id=0, has_side_effects=True, vmem_limit_bytes=room
        ),
    )(
        source, *[jnp.asarray(t) for t in tables],
        symbol_x[None], symbol_y[None], symbol_z[None],
    )
    return pl.pallas_call(
        finish,
        out_shape=jax.ShapeDtypeStruct((kl, jl, nz), jnp.float32),
        in_specs=[pl.BlockSpec(memory_space=pltpu.VMEM)] * 4,
        out_specs=pl.BlockSpec(memory_space=pltpu.HBM),
        scratch_shapes=[vmem((final, jl, nz), jnp.float32), dma((PIECES + final,))],
        compiler_params=pltpu.CompilerParams(vmem_limit_bytes=2**24),
    )(*[pltpu.with_memory_space_constraint(r, pltpu.VMEM) for r in ready])


def solution(mesh):
    placed = (P(None, "ya", "zb"), P(), P(), P())
    return jax.shard_map(
        functools.partial(body, mesh.shape["ya"], mesh.shape["zb"]),
        mesh=mesh, in_specs=placed, out_specs=P("ya", "zb", None), check_vma=False,
    )
```
